32 devices in a mesh: group: 8 (over y, x, core), ep: 4 (over z).
Axes of the slice: x: 2, y: 2, z: 4, core: 2. Of those that a mesh axis runs over, the one named last changes fastest.
Arguments:
- tokens: bfloat16 [1024, 3584], P(('group', 'ep')), may hold values from -6 to 6
- expert_ids: int32 [1024, 8], P(('group', 'ep')), may hold values from 0 to 31, as said below
- gate_scores: float32 [1024, 8], P(('group', 'ep')), may hold values from 0.05 to 0.35
- replica_pick: int32 [1024, 8], P(('group', 'ep')), may hold values from 0 to 8
- replica_hot: int32 [4], replicated, may hold values from 0 to 7
- gate_weight: bfloat16 [32, 3584, 1024], P(('group', 'ep')), may hold values from -0.09375 to 0.09375
- up_weight: bfloat16 [32, 3584, 1024], P(('group', 'ep')), may hold values from -0.09375 to 0.09375
- down_weight: bfloat16 [32, 1024, 3584], P(('group', 'ep')), may hold values from -0.1875 to 0.1875
Outputs:
- mixed: bfloat16 [1024, 3584], P(('group', 'ep'))
- slot_load: float32 [32, 2], P(('group', 'ep'))
The draws below stay inside these ranges and needn't reach their ends.
Inputs may be any that keep to these rules, and one draw needn't show every extreme that they name: `expert_ids`: each row names 8 different experts; in each aligned block of 16 rows (one micro-batch of one device) no expert is named by more than 5 rows, and the expert replica_hot[c] * 4 + c of each ep index c is named by exactly 5 rows.
All inputs are finite; a program needn't handle non-finite values.
Results may differ from the reference program's by a relative error of at most 0.0057.
Values may be sent and summed in bfloat16 or wider, within the bound.
A program may use at most 128 MiB of HBM per device.

```python
import jax
import jax.numpy as jnp
from jax import lax

D = 3584
FF = 1024
TOP = 8
MICRO = 2
MB_TOK = 16
EXPERTS = 32
TOKENS = 1024
MOST = 5
N_GROUP = 8
N_EP = 4


def hot_groups(key):
    base = jax.random.randint(jax.random.fold_in(key, 7), (N_EP,), 0, N_GROUP).astype(jnp.int32)
    where_top = jax.random.randint(jax.random.fold_in(key, 8), (), 0, N_EP).astype(jnp.int32)
    where_low = (where_top + 1) % N_EP
    base = base.at[where_top].set(N_GROUP - 1)
    base = base.at[where_low].set(0)
    return base.astype(jnp.int32)


def draw_replica_hot(key, part):
    return hot_groups(key)


def draw_expert_ids(key, part):
    hot_group = hot_groups(key)
    expert_range = jnp.arange(EXPERTS, dtype=jnp.int32)
    not_hot = 1 - (hot_group[expert_range % N_EP] == expert_range // N_EP).astype(jnp.int32)
    hot_pairs = N_EP * MOST
    rest_pairs = max(MB_TOK * TOP - hot_pairs, 1)
    rest_count = EXPERTS - N_EP
    row_index = jnp.arange(MB_TOK, dtype=jnp.int32)[:, None]
    col_index = jnp.arange(TOP, dtype=jnp.int32)[None, :]
    pair_index = col_index * MB_TOK + row_index
    rest_index = N_EP + jnp.maximum(pair_index - hot_pairs, 0) * rest_count // rest_pairs
    place = jnp.where(pair_index < hot_pairs, pair_index // MOST, rest_index).astype(jnp.int32)

    def one_block(block):
        shuffle = jax.random.permutation(jax.random.fold_in(key, 1000 + block), EXPERTS).astype(jnp.int32)
        ordering = shuffle[jnp.argsort(not_hot[shuffle], stable=True)]
        return ordering[place]
    blocks = jax.vmap(one_block)(jnp.arange(TOKENS // MB_TOK, dtype=jnp.int32))
    return blocks.reshape(TOKENS, TOP).astype(jnp.int32)


def with_ends(array, rng, least, largest):
    dims = array.shape
    spot = [jax.random.randint(jax.random.fold_in(rng, axis), (), 0, dims[axis]) for axis in range(len(dims))]
    array = array.at[tuple(spot)].set(least)
    longest = dims.index(max(dims))
    spot[longest] = (spot[longest] + 1) % dims[longest]
    return array.at[tuple(spot)].set(largest)


def levels(rng, dims, pieces, smallest, high):
    def one(dim, parts):
        draws = jax.random.uniform(jax.random.fold_in(jax.random.fold_in(rng, 6), dim), (parts,), jnp.float32, smallest / len(pieces), high / len(pieces))
        return jnp.repeat(jnp.exp(draws), dims[dim] // parts).reshape((-1,) + (1,) * (len(dims) - dim - 1))

    loudness = one(*pieces[0])
    for cut in pieces[1:]:
        loudness = loudness * one(*cut)
    return loudness


def bell_draw(own_key, shape, deviation, most, shards=(), held_as=jnp.bfloat16):
    result = jax.random.normal(own_key, shape, jnp.float32) * deviation
    if len(shards) > 0:
        result = levels(own_key, shape, shards, -0.22, 0.18) * result
    return jnp.clip(result, min=-most, max=most).astype(held_as)


def setup_inputs(seed: int = 0) -> dict:
    splits = jax.random.split(jax.random.key(seed), 9)
    tokens = bell_draw(splits[0], (TOKENS, D), 1.0, 6.0, ((0, 32),))
    expert_ids = draw_expert_ids(jax.random.fold_in(splits[8], 71), 0)
    gate_scores = jnp.clip(0.05 + 0.29999999 * jax.random.uniform(splits[2], (TOKENS, TOP), jnp.float32) ** levels(splits[2], (TOKENS, TOP), ((0, 32),), -0.2, 0.2), 0.05, 0.35)
    replica_pick = with_ends(jax.random.randint(splits[3], (TOKENS, TOP), 0, N_GROUP + 1), jax.random.fold_in(splits[3], 1), 0, N_GROUP).astype(jnp.int32)
    replica_hot = draw_replica_hot(jax.random.fold_in(splits[8], 71), 0)
    gate_weight = bell_draw(splits[5], (EXPERTS, D, FF), D ** -0.5, 0.09375, ((0, 32),))
    up_weight = bell_draw(splits[6], (EXPERTS, D, FF), D ** -0.5, 0.09375, ((0, 32),))
    down_weight = bell_draw(splits[7], (EXPERTS, FF, D), FF ** -0.5, 0.1875, ((0, 32),))
    return {"tokens": tokens, "expert_ids": expert_ids, "gate_scores": gate_scores, "replica_pick": replica_pick, "replica_hot": replica_hot, "gate_weight": gate_weight, "up_weight": up_weight, "down_weight": down_weight}


def expert_ffn(inputs, w_gate, w_up, w_down):
    gate_act = jnp.dot(inputs, w_gate, preferred_element_type=jnp.float32)
    up_act = jnp.dot(inputs, w_up, preferred_element_type=jnp.float32)
    hidden = (jax.nn.silu(gate_act) * up_act).astype(jnp.bfloat16)
    return jnp.dot(hidden, w_down, preferred_element_type=jnp.float32).astype(jnp.bfloat16)


def reference(tokens, expert_ids, gate_scores, replica_pick, replica_hot, gate_weight, up_weight, down_weight):
    flat_ids = expert_ids.reshape(-1).astype(jnp.int32)
    pair_count = flat_ids.shape[0]
    sort_order = jnp.argsort(flat_ids, stable=True).astype(jnp.int32)
    counts = jnp.zeros((EXPERTS,), jnp.int32).at[flat_ids].add(1)
    starts = (jnp.cumsum(counts) - counts).astype(jnp.int32)
    inverse = jnp.zeros((pair_count,), jnp.int32).at[sort_order].set(jnp.arange(pair_count, dtype=jnp.int32))
    pair_rank = (inverse - starts[flat_ids]).astype(jnp.int32)
    capacity = MICRO * MOST * EXPERTS
    sorted_tokens = jnp.concatenate([(sort_order // TOP).astype(jnp.int32), jnp.zeros((capacity,), jnp.int32)])

    def one_expert(expert):
        token_index = lax.dynamic_slice_in_dim(sorted_tokens, starts[expert], capacity)
        return expert_ffn(tokens[token_index], gate_weight[expert], up_weight[expert], down_weight[expert])

    expert_outs = lax.map(one_expert, jnp.arange(EXPERTS, dtype=jnp.int32))
    pair_outs = expert_outs[flat_ids, pair_rank].reshape(TOKENS, TOP, D).astype(jnp.float32)
    mixed = jnp.sum(gate_scores[:, :, None] * pair_outs, axis=1).astype(jnp.bfloat16)

    column = flat_ids % N_EP
    home_group = flat_ids // N_EP
    pick_flat = replica_pick.reshape(-1).astype(jnp.int32)
    replicated = (replica_hot[column] == home_group) & (pick_flat < N_GROUP)
    device = jnp.where(replicated, pick_flat, home_group) * N_EP + column
    slot_key = (device * 2 + replicated.astype(jnp.int32)).astype(jnp.int32)
    slot_load = jnp.zeros((2 * EXPERTS,), jnp.float32).at[slot_key].add(1.0).reshape(EXPERTS, 2) / TOP
    return mixed, slot_load
```

```python
import jax
import jax.numpy as jnp
from jax import lax
from jax.sharding import PartitionSpec as P

AXES = ("group", "ep")


def body(
    tokens, expert_ids, gate_scores, replica_pick, replica_hot, gate_weight, up_weight, down_weight
):
    ngroup = lax.axis_size("group")
    ep_count = lax.axis_size("ep")
    device_count = ngroup * ep_count
    group_index = lax.axis_index("group")
    ep_index = lax.axis_index("ep")
    me = group_index * ep_count + ep_index
    tok_dev, width = tokens.shape
    top_count = expert_ids.shape[1]
    micro_len = tok_dev // 2
    most = (micro_len * top_count + device_count - 1) // device_count + 1
    capacity = 2 * most * device_count

    routing = jnp.concatenate(
        [expert_ids.astype(jnp.float32), replica_pick.astype(jnp.float32), gate_scores], axis=1
    )
    routing = lax.all_gather(routing, AXES, axis=0, tiled=True)
    every = lax.all_gather(tokens, AXES, axis=0, tiled=True)
    ids = routing[:, :top_count].astype(jnp.int32)
    picks = routing[:, top_count : 2 * top_count].astype(jnp.int32)
    gates = routing[:, 2 * top_count :]

    hot = replica_hot[ep_index]
    in_column = ids % ep_count == ep_index
    replicated = in_column & (ids // ep_count == hot) & (picks < ngroup)
    primary_load = jnp.sum(((ids == me) & ~replicated).astype(jnp.float32))
    replica_load = jnp.sum((replicated & (picks == group_index)).astype(jnp.float32))
    loads = jnp.stack([primary_load, replica_load])[None, :] / top_count

    chosen = ids == me
    mask = jnp.any(chosen, axis=1)
    scale = jnp.sum(jnp.where(chosen, gates, 0.0), axis=1)
    place = jnp.where(mask, jnp.cumsum(mask.astype(jnp.int32)) - 1, -1)
    spot = place[None, :] == jnp.arange(capacity, dtype=jnp.int32)[:, None]
    select = spot.astype(jnp.bfloat16)
    row_scale = jnp.sum(jnp.where(spot, scale[None, :], 0.0), axis=1)
    picked = jnp.dot(select, every, preferred_element_type=jnp.float32).astype(jnp.bfloat16)
    gate_act = jnp.dot(picked, gate_weight[0], preferred_element_type=jnp.float32)
    up_act = jnp.dot(picked, up_weight[0], preferred_element_type=jnp.float32)
    hidden = (jax.nn.silu(gate_act) * up_act).astype(jnp.bfloat16)
    pair_out = jnp.dot(hidden, down_weight[0], preferred_element_type=jnp.float32)
    scaled = (pair_out * row_scale[:, None]).astype(jnp.bfloat16)
    spread = jnp.dot(select.T, scaled, preferred_element_type=jnp.float32).astype(jnp.bfloat16)
    mixed = lax.psum_scatter(spread, AXES, scatter_dimension=0, tiled=True)
    return mixed, loads


def solution(mesh):
    rows = P(AXES, None)
    return jax.shard_map(
        body,
        mesh=mesh,
        in_specs=(rows, rows, rows, rows, P(), P(AXES, None, None), P(AXES, None, None), P(AXES, None, None)),
        out_specs=(rows, rows),
        check_vma=False,
    )
```

```python
import functools

import jax
import jax.numpy as jnp
from jax import lax
from jax.experimental import pallas as pl
from jax.experimental.pallas import tpu as pltpu
from jax.sharding import PartitionSpec as P

AXES = ("group", "ep")
MESH = pl.DeviceIdType.MESH


def place_of(nplane, nep):
    group = lax.axis_index("group")
    ep = lax.axis_index("ep")
    core = lax.rem(group, 2)
    plane = lax.div(group, 2)

    def plane_peer(step):
        other = lax.rem(plane + step, nplane)
        return other, (other * 2 + core, ep)

    def ep_peer(step):
        other = lax.rem(ep + step, nep)
        return other, (group, other)

    return plane, ep, plane_peer, ep_peer


def greet(nplane, nep, plane_peer, ep_peer):
    barrier = pltpu.get_barrier_semaphore()
    for step in range(1, nplane):
        pl.semaphore_signal(barrier, inc=1, device_id=plane_peer(step)[1], device_id_type=MESH)
    for step in range(1, nep):
        pl.semaphore_signal(barrier, inc=1, device_id=ep_peer(step)[1], device_id_type=MESH)
    pl.semaphore_wait(barrier, nplane + nep - 2)


def gather_kernel(nplane, nep, cut, x_ref, out_ref, own_sem, send_a, recv_a, send_b, recv_b):
    plane, ep, plane_peer, ep_peer = place_of(nplane, nep)
    width = x_ref.shape[1]
    cols_a, cols_b = pl.ds(0, cut), pl.ds(cut, width - cut)
    own = pltpu.make_async_copy(x_ref, out_ref.at[plane, ep], own_sem)
    own.start()
    greet(nplane, nep, plane_peer, ep_peer)
    sends = []

    def copy(src, p, e, cols, send, recv, target):
        return pltpu.make_async_remote_copy(
            src_ref=src.at[:, cols],
            dst_ref=out_ref.at[p, e, :, cols],
            send_sem=send,
            recv_sem=recv.at[p * nep + e],
            device_id=target,
            device_id_type=MESH,
        )

    used = {"a": 0, "b": 0}

    def push(src, p, e, half, target):
        cols, send, recv = (cols_a, send_a, recv_a) if half == "a" else (cols_b, send_b, recv_b)
        made = copy(src, p, e, cols, send.at[used[half]], recv, target)
        used[half] += 1
        made.start()
        sends.append(made)

    def arrived(p, e, half):
        cols, send, recv = (cols_a, send_a, recv_a) if half == "a" else (cols_b, send_b, recv_b)
        copy(out_ref.at[p, e], p, e, cols, send.at[0], recv, ep_peer(1)[1]).wait_recv()

    for step in range(1, nep):
        push(x_ref, plane, ep, "a", ep_peer(step)[1])
    for step in range(1, nplane):
        push(x_ref, plane, ep, "b", plane_peer(step)[1])
    for step in range(1, nplane):
        push(x_ref, plane, ep, "a", plane_peer(step)[1])
    for step in range(1, nep):
        push(x_ref, plane, ep, "b", ep_peer(step)[1])
    for back in range(1, max(nplane, nep)):
        if back < nep:
            source = lax.rem(ep + nep - back, nep)
            arrived(plane, source, "a")
            for step in range(1, nplane):
                push(out_ref.at[plane, source], plane, source, "a", plane_peer(step)[1])
        if back < nplane:
            source = lax.rem(plane + nplane - back, nplane)
            arrived(source, ep, "b")
            for step in range(1, nep):
                push(out_ref.at[source, ep], source, ep, "b", ep_peer(step)[1])
    for p_back in range(nplane):
        for e_back in range(nep):
            p = lax.rem(plane + nplane - p_back, nplane)
            e = lax.rem(ep + nep - e_back, nep)
            if p_back > 0:
                arrived(p, e, "a")
            if e_back > 0:
                arrived(p, e, "b")
    for made in sends:
        made.wait_send()
    own.wait()


def gather_plane(tokens, nplane, nep, cut):
    rows, width = tokens.shape
    count = nplane * nep
    return pl.pallas_call(
        functools.partial(gather_kernel, nplane, nep, cut),
        out_shape=jax.ShapeDtypeStruct((nplane, nep, rows, width), tokens.dtype),
        in_specs=[pl.BlockSpec(memory_space=pltpu.VMEM)],
        out_specs=pl.BlockSpec(memory_space=pltpu.VMEM),
        scratch_shapes=[pltpu.SemaphoreType.DMA(())] + [pltpu.SemaphoreType.DMA((count,))] * 4,
        compiler_params=pltpu.CompilerParams(collective_id=0, has_side_effects=True),
    )(tokens)


def scatter_kernel(
    nplane, nep, cut, part_ref, out_ref,
    land_a1, land_b1, mid_a, mid_b, land_a2, land_b2,
    send_a1, recv_a1, send_b1, recv_b1, send_a2, recv_a2, send_b2, recv_b2,
):
    plane, ep, plane_peer, ep_peer = place_of(nplane, nep)
    width = out_ref.shape[1]
    cols_a, cols_b = pl.ds(0, cut), pl.ds(cut, width - cut)
    greet(nplane, nep, plane_peer, ep_peer)

    def move(src, dst, send, recv, target):
        made = pltpu.make_async_remote_copy(
            src_ref=src, dst_ref=dst, send_sem=send, recv_sem=recv, device_id=target, device_id_type=MESH
        )
        made.start()
        return made

    first_a, first_b = {}, {}
    for item in range(1, max(nplane, nep) + 1):
        if item <= nep:
            e = lax.rem(ep + item, nep)
            for step in range(1, nplane):
                p, target = plane_peer(step)
                spot = (step - 1) * nep + item - 1
                first_a[item, step] = move(
                    part_ref.at[p, e, :, cols_a], land_a1.at[step - 1, item - 1],
                    send_a1.at[spot], recv_a1.at[spot], target,
                )
        if item <= nplane:
            p = lax.rem(plane + item, nplane)
            for step in range(1, nep):
                e, target = ep_peer(step)
                spot = (step - 1) * nplane + item - 1
                first_b[item, step] = move(
                    part_ref.at[p, e, :, cols_b], land_b1.at[step - 1, item - 1],
                    send_b1.at[spot], recv_b1.at[spot], target,
                )
    second_a, second_b = [], []
    for item in range(1, max(nplane, nep) + 1):
        if item <= nep:
            e, target = ep_peer(item)
            total = part_ref[plane, e, :, cols_a].astype(jnp.float32)
            for step in range(1, nplane):
                first_a[item, step].wait_recv()
                total = total + land_a1[step - 1, item - 1].astype(jnp.float32)
            if item < nep:
                mid_a[item - 1] = total.astype(mid_a.dtype)
                second_a.append(
                    move(mid_a.at[item - 1], land_a2.at[item - 1], send_a2.at[item - 1], recv_a2.at[item - 1], target)
                )
            else:
                total_a = total
        if item <= nplane:
            p, target = plane_peer(item)
            total = part_ref[p, ep, :, cols_b].astype(jnp.float32)
            for step in range(1, nep):
                first_b[item, step].wait_recv()
                total = total + land_b1[step - 1, item - 1].astype(jnp.float32)
            if item < nplane:
                mid_b[item - 1] = total.astype(mid_b.dtype)
                second_b.append(
                    move(mid_b.at[item - 1], land_b2.at[item - 1], send_b2.at[item - 1], recv_b2.at[item - 1], target)
                )
            else:
                total_b = total
    for index, made in enumerate(second_a):
        made.wait_recv()
        total_a = total_a + land_a2[index].astype(jnp.float32)
    out_ref[:, cols_a] = total_a.astype(out_ref.dtype)
    for index, made in enumerate(second_b):
        made.wait_recv()
        total_b = total_b + land_b2[index].astype(jnp.float32)
    out_ref[:, cols_b] = total_b.astype(out_ref.dtype)
    for made in list(first_a.values()) + list(first_b.values()) + second_a + second_b:
        made.wait_send()


def scatter_plane(parts, cut):
    nplane, nep, rows, width = parts.shape
    rest = width - cut
    kind = parts.dtype
    dma = pltpu.SemaphoreType.DMA
    pairs_a, pairs_b = (nplane - 1) * nep, (nep - 1) * nplane
    return pl.pallas_call(
        functools.partial(scatter_kernel, nplane, nep, cut),
        out_shape=jax.ShapeDtypeStruct((rows, width), kind),
        in_specs=[pl.BlockSpec(memory_space=pltpu.VMEM)],
        out_specs=pl.BlockSpec(memory_space=pltpu.VMEM),
        scratch_shapes=[
            pltpu.VMEM((nplane - 1, nep, rows, cut), kind),
            pltpu.VMEM((nep - 1, nplane, rows, rest), kind),
            pltpu.VMEM((nep - 1, rows, cut), kind),
            pltpu.VMEM((nplane - 1, rows, rest), kind),
            pltpu.VMEM((nep - 1, rows, cut), kind),
            pltpu.VMEM((nplane - 1, rows, rest), kind),
            dma((pairs_a,)), dma((pairs_a,)), dma((pairs_b,)), dma((pairs_b,)),
            dma((nep - 1,)), dma((nep - 1,)), dma((nplane - 1,)), dma((nplane - 1,)),
        ],
        compiler_params=pltpu.CompilerParams(collective_id=1, has_side_effects=True),
    )(parts)


def body(
    tokens, expert_ids, gate_scores, replica_pick, replica_hot, gate_weight, up_weight, down_weight
):
    ngroup = lax.axis_size("group")
    nep = lax.axis_size("ep")
    nplane = ngroup // 2
    device_count = ngroup * nep
    group_index = lax.axis_index("group")
    ep_index = lax.axis_index("ep")
    core = group_index % 2
    me = group_index * nep + ep_index
    partner = (group_index + 1 - 2 * core) * nep + ep_index
    tok_dev, width = tokens.shape
    top_count = expert_ids.shape[1]
    most = (tok_dev // 2 * top_count + device_count - 1) // device_count + 1
    capacity = 2 * most * nplane * nep
    cut = width // 256 * 128

    routing = jnp.concatenate(
        [expert_ids.astype(jnp.float32), replica_pick.astype(jnp.float32), gate_scores], axis=1
    )
    routing = lax.all_gather(routing, AXES, axis=0, tiled=True)
    every = gather_plane(tokens, nplane, nep, cut).reshape(nplane * nep * tok_dev, width)

    ids = routing[:, :top_count].astype(jnp.int32)
    picks = routing[:, top_count : 2 * top_count].astype(jnp.int32)
    hot = replica_hot[ep_index]
    replicated = (ids % nep == ep_index) & (ids // nep == hot) & (picks < ngroup)
    primary_load = jnp.sum(((ids == me) & ~replicated).astype(jnp.float32))
    replica_load = jnp.sum((replicated & (picks == group_index)).astype(jnp.float32))
    loads = jnp.stack([primary_load, replica_load])[None, :] / top_count

    mine = routing.reshape(nplane, 2, nep * tok_dev, routing.shape[1])
    mine = lax.dynamic_index_in_dim(mine, core, 1, keepdims=False).reshape(-1, routing.shape[1])
    my_ids = mine[:, :top_count].astype(jnp.int32)
    my_gates = mine[:, 2 * top_count :]

    def spots(expert):
        chosen = my_ids == expert
        mask = jnp.any(chosen, axis=1)
        scale = jnp.sum(jnp.where(chosen, my_gates, 0.0), axis=1)
        place = jnp.where(mask, jnp.cumsum(mask.astype(jnp.int32)) - 1, -1)
        spot = place[None, :] == jnp.arange(capacity, dtype=jnp.int32)[:, None]
        return spot, jnp.sum(jnp.where(spot, scale[None, :], 0.0), axis=1)

    spot_me, scale_me = spots(me)
    spot_other, scale_other = spots(partner)
    select = jnp.concatenate([spot_me, spot_other], axis=0).astype(jnp.bfloat16)
    row_scale = jnp.concatenate([scale_me, scale_other], axis=0)
    swap = [(index, index ^ 1) for index in range(ngroup)]

    picked = jnp.dot(select, every, preferred_element_type=jnp.float32).astype(jnp.bfloat16)
    inputs = jnp.concatenate(
        [picked[:capacity], lax.ppermute(picked[capacity:], "group", swap)], axis=0
    )
    gate_act = jnp.dot(inputs, gate_weight[0], preferred_element_type=jnp.float32)
    up_act = jnp.dot(inputs, up_weight[0], preferred_element_type=jnp.float32)
    hidden = (jax.nn.silu(gate_act) * up_act).astype(jnp.bfloat16)
    pair_out = jnp.dot(hidden, down_weight[0], preferred_element_type=jnp.float32).astype(jnp.bfloat16)
    pairs = jnp.concatenate(
        [pair_out[:capacity], lax.ppermute(pair_out[capacity:], "group", swap)], axis=0
    )
    scaled = (pairs.astype(jnp.float32) * row_scale[:, None]).astype(jnp.bfloat16)
    spread = lax.dot_general(
        select, scaled, (((0,), (0,)), ((), ())), preferred_element_type=jnp.float32
    ).astype(jnp.bfloat16)
    mixed = scatter_plane(spread.reshape(nplane, nep, tok_dev, width), cut)
    return mixed, loads


def solution(mesh):
    rows = P(AXES, None)
    weights = P(AXES, None, None)
    return jax.shard_map(
        body,
        mesh=mesh,
        in_specs=(rows, rows, rows, rows, P(), weights, weights, weights),
        out_specs=(rows, rows),
        check_vma=False,
    )
```

```python
import functools

import jax
import jax.numpy as jnp
from jax import lax
from jax.experimental import pallas as pl
from jax.experimental.pallas import tpu as pltpu
from jax.sharding import PartitionSpec as P

AXES = ("group", "ep")
MESH = pl.DeviceIdType.MESH


def place_of(nplane, nep):
    group = lax.axis_index("group")
    ep = lax.axis_index("ep")
    core = lax.rem(group, 2)
    plane = lax.div(group, 2)

    def plane_peer(step):
        other = lax.rem(plane + step, nplane)
        return other, (other * 2 + core, ep)

    def ep_peer(step):
        other = lax.rem(ep + step, nep)
        return other, (group, other)

    return plane, ep, plane_peer, ep_peer


def greet(nplane, nep, plane_peer, ep_peer):
    barrier = pltpu.get_barrier_semaphore()
    for step in range(1, nplane):
        pl.semaphore_signal(barrier, inc=1, device_id=plane_peer(step)[1], device_id_type=MESH)
    for step in range(1, nep):
        pl.semaphore_signal(barrier, inc=1, device_id=ep_peer(step)[1], device_id_type=MESH)
    pl.semaphore_wait(barrier, nplane + nep - 2)


def gather_kernel(
    nplane, nep, cut, x_ref, note_ref, out_ref, notes_ref,
    own_sem, send_a, recv_a, send_b, recv_b, right_a, left_a, right_b, left_b, note_send, note_recv,
):
    plane, ep, plane_peer, ep_peer = place_of(nplane, nep)
    group = lax.axis_index("group")
    me = group * nep + ep
    total = 2 * nplane * nep
    width = x_ref.shape[1]
    cols = {"a": pl.ds(0, cut), "b": pl.ds(cut, width - cut)}
    recv = {"a": recv_a, "b": recv_b}
    rights = {"a": right_a, "b": right_b}
    lefts = {"a": left_a, "b": left_b}
    own = pltpu.make_async_copy(x_ref, out_ref.at[plane, ep], own_sem.at[0])
    own.start()
    own_note = pltpu.make_async_copy(note_ref, notes_ref.at[me], own_sem.at[1])
    own_note.start()

    barrier = pltpu.get_barrier_semaphore()
    for step in range(1, total):
        other = lax.rem(me + step, total)
        pl.semaphore_signal(
            barrier, inc=1, device_id=(lax.div(other, nep), lax.rem(other, nep)), device_id_type=MESH
        )
    pl.semaphore_wait(barrier, total - 1)

    def copy(src, p, e, half, send, target):
        return pltpu.make_async_remote_copy(
            src_ref=src.at[:, cols[half]],
            dst_ref=out_ref.at[p, e, :, cols[half]],
            send_sem=send,
            recv_sem=recv[half].at[p * nep + e],
            device_id=target,
            device_id_type=MESH,
        )

    sends = []
    used = {"a": 0, "b": 0}

    def push(src, p, e, half):
        send = send_a if half == "a" else send_b
        for step in range(1, nplane):
            made = copy(src, p, e, half, send.at[used[half]], plane_peer(step)[1])
            used[half] += 1
            made.start()
            sends.append(made)

    def arrived(p, e, half):
        copy(out_ref.at[p, e], p, e, half, send_a.at[0], ep_peer(1)[1]).wait_recv()

    def to_right(src, p, e, half):
        return copy(src, p, e, half, rights[half].at[p * nep + e], (group, lax.rem(ep + 1, nep)))

    def to_left(src, p, e, half):
        return copy(src, p, e, half, lefts[half].at[p * nep + e], (group, lax.rem(ep + nep - 1, nep)))

    has_right, has_left = ep < nep - 1, ep > 0

    def both_ways(src, p, half):
        @pl.when(has_right)
        def _():
            to_right(src, p, ep, half).start()

        @pl.when(has_left)
        def _():
            to_left(src, p, ep, half).start()

    def chain(p, back, half):
        @pl.when(ep - back >= 0)
        def _():
            arrived(p, ep - back, half)

            @pl.when(has_right)
            def _():
                to_right(out_ref.at[p, ep - back], p, ep - back, half).start()

        @pl.when(ep + back < nep)
        def _():
            arrived(p, ep + back, half)

            @pl.when(has_left)
            def _():
                to_left(out_ref.at[p, ep + back], p, ep + back, half).start()

    def chain_end(p, back, half):
        @pl.when((ep - back >= 0) & has_right)
        def _():
            to_right(out_ref.at[p, ep - back], p, ep - back, half).wait_send()

        @pl.when((ep + back < nep) & has_left)
        def _():
            to_left(out_ref.at[p, ep + back], p, ep + back, half).wait_send()

    def note(source, step, target):
        return pltpu.make_async_remote_copy(
            src_ref=note_ref,
            dst_ref=notes_ref.at[source],
            send_sem=note_send.at[step],
            recv_sem=note_recv.at[source],
            device_id=(lax.div(target, nep), lax.rem(target, nep)),
            device_id_type=MESH,
        )

    both_ways(x_ref, plane, "a")
    push(x_ref, plane, ep, "b")
    push(x_ref, plane, ep, "a")
    both_ways(x_ref, plane, "b")
    for step in range(1, total):
        note(me, step, lax.rem(me + step, total)).start()
    for back in range(1, max(nplane, nep)):
        if back < nep:
            chain(plane, back, "a")
        if back < nplane:
            source = lax.rem(plane + nplane - back, nplane)
            arrived(source, ep, "b")
            both_ways(out_ref.at[source, ep], source, "b")
        if back < nep:
            left_in, right_in = ep - back >= 0, ep + back < nep

            @pl.when(left_in)
            def _():
                for step in range(1, nplane):
                    copy(
                        out_ref.at[plane, ep - back], plane, ep - back, "a",
                        send_a.at[(nplane - 1) * back + step - 1], plane_peer(step)[1],
                    ).start()

            @pl.when(right_in)
            def _():
                for step in range(1, nplane):
                    copy(
                        out_ref.at[plane, ep + back], plane, ep + back, "a",
                        send_a.at[(nplane - 1) * (nep + back) + step - 1], plane_peer(step)[1],
                    ).start()
    for back in range(1, nep):
        for p_back in range(nplane):
            chain(lax.rem(plane + nplane - p_back, nplane), back, "b")
    for p_back in range(1, nplane):
        p = lax.rem(plane + nplane - p_back, nplane)
        for e in range(nep):
            arrived(p, e, "a")
    for step in range(1, total):
        source = lax.rem(me + total - step, total)
        note(source, step, lax.rem(me + 1, total)).wait_recv()
    for made in sends:
        made.wait_send()
    for back in range(1, nep):
        @pl.when(ep - back >= 0)
        def _():
            for step in range(1, nplane):
                copy(
                    out_ref.at[plane, ep - back], plane, ep - back, "a",
                    send_a.at[(nplane - 1) * back + step - 1], plane_peer(step)[1],
                ).wait_send()

        @pl.when(ep + back < nep)
        def _():
            for step in range(1, nplane):
                copy(
                    out_ref.at[plane, ep + back], plane, ep + back, "a",
                    send_a.at[(nplane - 1) * (nep + back) + step - 1], plane_peer(step)[1],
                ).wait_send()

    for back in range(nep):
        for half in ("a", "b"):
            for p_back in range(nplane if half == "b" else 1):
                p = lax.rem(plane + nplane - p_back, nplane)
                if back == 0:
                    @pl.when(has_right)
                    def _():
                        to_right(x_ref, p, ep, half).wait_send()

                    @pl.when(has_left)
                    def _():
                        to_left(x_ref, p, ep, half).wait_send()
                else:
                    chain_end(p, back, half)
    for step in range(1, total):
        note(me, step, lax.rem(me + step, total)).wait_send()
    own.wait()
    own_note.wait()


def gather_plane(tokens, note, nplane, nep, cut):
    rows, width = tokens.shape
    count = nplane * nep
    dma = pltpu.SemaphoreType.DMA
    vmem = pl.BlockSpec(memory_space=pltpu.VMEM)
    return pl.pallas_call(
        functools.partial(gather_kernel, nplane, nep, cut),
        out_shape=[
            jax.ShapeDtypeStruct((nplane, nep, rows, width), tokens.dtype),
            jax.ShapeDtypeStruct((2 * count,) + note.shape, note.dtype),
        ],
        in_specs=[vmem, vmem],
        out_specs=[vmem, vmem],
        scratch_shapes=[
            dma((2,)),
            dma((2 * (nplane - 1) * nep,)), dma((count,)), dma((nplane - 1,)), dma((count,)),
            dma((count,)), dma((count,)), dma((count,)), dma((count,)),
            dma((2 * count,)), dma((2 * count,)),
        ],
        compiler_params=pltpu.CompilerParams(collective_id=0, has_side_effects=True),
    )(tokens, note)


def scatter_kernel(
    nplane, nep, cut, part_ref, out_ref,
    land_a1, land_b1, mid_a, mid_b, land_a2, land_b2,
    send_a1, recv_a1, send_b1, recv_b1, send_a2, recv_a2, send_b2, recv_b2,
):
    plane, ep, plane_peer, ep_peer = place_of(nplane, nep)
    width = out_ref.shape[1]
    cols_a, cols_b = pl.ds(0, cut), pl.ds(cut, width - cut)
    greet(nplane, nep, plane_peer, ep_peer)

    def move(src, dst, send, recv, target):
        made = pltpu.make_async_remote_copy(
            src_ref=src, dst_ref=dst, send_sem=send, recv_sem=recv, device_id=target, device_id_type=MESH
        )
        made.start()
        return made

    first_a, first_b = {}, {}
    for item in range(1, max(nplane, nep) + 1):
        if item <= nep:
            e = lax.rem(ep + item, nep)
            for step in range(1, nplane):
                p, target = plane_peer(step)
                spot = (step - 1) * nep + item - 1
                first_a[item, step] = move(
                    part_ref.at[p, e, :, cols_a], land_a1.at[step - 1, item - 1],
                    send_a1.at[spot], recv_a1.at[spot], target,
                )
        if item <= nplane:
            p = lax.rem(plane + item, nplane)
            for step in range(1, nep):
                e, target = ep_peer(step)
                spot = (step - 1) * nplane + item - 1
                first_b[item, step] = move(
                    part_ref.at[p, e, :, cols_b], land_b1.at[step - 1, item - 1],
                    send_b1.at[spot], recv_b1.at[spot], target,
                )
    second_a, second_b = [], []
    for item in range(1, max(nplane, nep) + 1):
        if item <= nep:
            e, target = ep_peer(item)
            total = part_ref[plane, e, :, cols_a].astype(jnp.float32)
            for step in range(1, nplane):
                first_a[item, step].wait_recv()
                total = total + land_a1[step - 1, item - 1].astype(jnp.float32)
            if item < nep:
                mid_a[item - 1] = total.astype(mid_a.dtype)
                second_a.append(
                    move(mid_a.at[item - 1], land_a2.at[item - 1], send_a2.at[item - 1], recv_a2.at[item - 1], target)
                )
            else:
                total_a = total
        if item <= nplane:
            p, target = plane_peer(item)
            total = part_ref[p, ep, :, cols_b].astype(jnp.float32)
            for step in range(1, nep):
                first_b[item, step].wait_recv()
                total = total + land_b1[step - 1, item - 1].astype(jnp.float32)
            if item < nplane:
                mid_b[item - 1] = total.astype(mid_b.dtype)
                second_b.append(
                    move(mid_b.at[item - 1], land_b2.at[item - 1], send_b2.at[item - 1], recv_b2.at[item - 1], target)
                )
            else:
                total_b = total
    for index, made in enumerate(second_a):
        made.wait_recv()
        total_a = total_a + land_a2[index].astype(jnp.float32)
    out_ref[:, cols_a] = total_a.astype(out_ref.dtype)
    for index, made in enumerate(second_b):
        made.wait_recv()
        total_b = total_b + land_b2[index].astype(jnp.float32)
    out_ref[:, cols_b] = total_b.astype(out_ref.dtype)
    for made in list(first_a.values()) + list(first_b.values()) + second_a + second_b:
        made.wait_send()


def scatter_plane(parts, cut):
    nplane, nep, rows, width = parts.shape
    rest = width - cut
    kind = parts.dtype
    dma = pltpu.SemaphoreType.DMA
    pairs_a, pairs_b = (nplane - 1) * nep, (nep - 1) * nplane
    return pl.pallas_call(
        functools.partial(scatter_kernel, nplane, nep, cut),
        out_shape=jax.ShapeDtypeStruct((rows, width), kind),
        in_specs=[pl.BlockSpec(memory_space=pltpu.VMEM)],
        out_specs=pl.BlockSpec(memory_space=pltpu.VMEM),
        scratch_shapes=[
            pltpu.VMEM((nplane - 1, nep, rows, cut), kind),
            pltpu.VMEM((nep - 1, nplane, rows, rest), kind),
            pltpu.VMEM((nep - 1, rows, cut), kind),
            pltpu.VMEM((nplane - 1, rows, rest), kind),
            pltpu.VMEM((nep - 1, rows, cut), kind),
            pltpu.VMEM((nplane - 1, rows, rest), kind),
            dma((pairs_a,)), dma((pairs_a,)), dma((pairs_b,)), dma((pairs_b,)),
            dma((nep - 1,)), dma((nep - 1,)), dma((nplane - 1,)), dma((nplane - 1,)),
        ],
        compiler_params=pltpu.CompilerParams(collective_id=1, has_side_effects=True),
    )(parts)


def body(
    tokens, expert_ids, gate_scores, replica_pick, replica_hot, gate_weight, up_weight, down_weight
):
    ngroup = lax.axis_size("group")
    nep = lax.axis_size("ep")
    nplane = ngroup // 2
    device_count = ngroup * nep
    group_index = lax.axis_index("group")
    ep_index = lax.axis_index("ep")
    core = group_index % 2
    me = group_index * nep + ep_index
    partner = (group_index + 1 - 2 * core) * nep + ep_index
    tok_dev, width = tokens.shape
    top_count = expert_ids.shape[1]
    most = (tok_dev // 2 * top_count + device_count - 1) // device_count + 1
    capacity = 2 * most * nplane * nep
    cut = width // 256 * 128
    back_cut = width * 11 // 14 // 128 * 128

    coded = expert_ids * (ngroup + 1) + replica_pick
    note = jnp.concatenate([coded.astype(jnp.float32), gate_scores], axis=1).reshape(-1, 128)
    every, notes = gather_plane(tokens, note, nplane, nep, cut)
    every = every.reshape(nplane * nep * tok_dev, width)
    routing = notes.reshape(device_count * tok_dev, 2 * top_count)
    coded = routing[:, :top_count].astype(jnp.int32)
    ids = coded // (ngroup + 1)
    picks = coded % (ngroup + 1)
    hot = replica_hot[ep_index]
    replicated = (ids % nep == ep_index) & (ids // nep == hot) & (picks < ngroup)
    primary_load = jnp.sum(((ids == me) & ~replicated).astype(jnp.float32))
    replica_load = jnp.sum((replicated & (picks == group_index)).astype(jnp.float32))
    loads = jnp.stack([primary_load, replica_load])[None, :] / top_count

    mine = routing.reshape(nplane, 2, nep * tok_dev, 2 * top_count)
    mine = lax.dynamic_index_in_dim(mine, core, 1, keepdims=False).reshape(-1, 2 * top_count)
    my_ids = mine[:, :top_count].astype(jnp.int32) // (ngroup + 1)
    my_gates = mine[:, top_count:]

    def spots(expert):
        chosen = my_ids == expert
        mask = jnp.any(chosen, axis=1)
        scale = jnp.sum(jnp.where(chosen, my_gates, 0.0), axis=1)
        place = jnp.where(mask, jnp.cumsum(mask.astype(jnp.int32)) - 1, -1)
        spot = place[None, :] == jnp.arange(capacity, dtype=jnp.int32)[:, None]
        return spot, jnp.sum(jnp.where(spot, scale[None, :], 0.0), axis=1)

    spot_me, scale_me = spots(me)
    spot_other, scale_other = spots(partner)
    select = jnp.concatenate([spot_me, spot_other], axis=0).astype(jnp.bfloat16)
    row_scale = jnp.concatenate([scale_me, scale_other], axis=0)
    swap = [(index, index ^ 1) for index in range(ngroup)]

    picked = jnp.dot(select, every, preferred_element_type=jnp.float32).astype(jnp.bfloat16)
    inputs = jnp.concatenate(
        [picked[:capacity], lax.ppermute(picked[capacity:], "group", swap)], axis=0
    )
    gate_act = jnp.dot(inputs, gate_weight[0], preferred_element_type=jnp.float32)
    up_act = jnp.dot(inputs, up_weight[0], preferred_element_type=jnp.float32)
    hidden = (jax.nn.silu(gate_act) * up_act).astype(jnp.bfloat16)
    pair_out = jnp.dot(hidden, down_weight[0], preferred_element_type=jnp.float32).astype(jnp.bfloat16)
    pairs = jnp.concatenate(
        [pair_out[:capacity], lax.ppermute(pair_out[capacity:], "group", swap)], axis=0
    )
    scaled = (pairs.astype(jnp.float32) * row_scale[:, None]).astype(jnp.bfloat16)
    spread = lax.dot_general(
        select, scaled, (((0,), (0,)), ((), ())), preferred_element_type=jnp.float32
    ).astype(jnp.bfloat16)
    mixed = scatter_plane(spread.reshape(nplane, nep, tok_dev, width), back_cut)
    return mixed, loads


def solution(mesh):
    rows = P(AXES, None)
    weights = P(AXES, None, None)
    return jax.shard_map(
        body,
        mesh=mesh,
        in_specs=(rows, rows, rows, rows, P(), weights, weights, weights),
        out_specs=(rows, rows),
        check_vma=False,
    )
```
